32 devices in a mesh: grp: 2 (over y), lat: 4 (over z), lon: 2 (over x), ch: 2 (over core).
Axes of the slice: x: 2, y: 2, z: 4, core: 2. Of those that a mesh axis runs over, the one named last changes fastest.
Arguments:
- noisy_state: bfloat16 [256, 32, 512], P(('grp', 'ch'), 'lat', 'lon'), parts along dimension 0, may hold values from -6 to 6
- kernel_in: bfloat16 [3, 3, 128, 128], replicated, may hold values from -0.1875 to 0.1875
- bias_in: float32 [128], replicated, may hold values from -4 to 4
- kernel_out: bfloat16 [3, 3, 128, 128], replicated, may hold values from -0.1875 to 0.1875
- interp_weight: bfloat16 [64, 128, 128], P(('grp', 'lat', 'lon')), parts along dimension 0, may hold values from -0.5 to 0.5
- observed: bfloat16 [64, 128, 128], P(('grp', 'lat', 'lon'), 'ch'), parts along dimension 0, may hold values from -6 to 6
- obs_precision: bfloat16 [64, 128], P(('grp', 'lat', 'lon')), parts along dimension 0, may hold values from 0.29882812 to 3
- dest_tile: int32 [64], P(('grp', 'lat', 'lon')), parts along dimension 0, may hold values from 0 to 3, as said below
- row_offset: int32 [64], P(('grp', 'lat', 'lon')), parts along dimension 0, may hold values from 0 to 4
- col_offset: int32 [64], P(('grp', 'lat', 'lon')), parts along dimension 0, may hold values from 0 to 224
Outputs:
- next_state: float32 [256, 32, 512], P(('grp', 'ch'), 'lat', 'lon'), parts along dimension 0
- innovation: bfloat16 [64, 128, 128], P(('grp', 'lat', 'lon'), 'ch'), parts along dimension 0
The draws below stay inside these ranges and needn't reach their ends.
There are 2 independent parts, one for each index of `grp`. The reference program is written for one: setup_inputs(seed, part) draws one part's arguments, and reference() takes and returns one part's arrays. A program takes and returns all parts, laid end to end along the dimension named above; an argument that names none is the same for every part. Nothing has to cross between parts.
Inputs may be any that keep to these rules, and one draw needn't show every extreme that they name: `dest_tile`: the 4 blocks of one device name any one latitude tile at most 2 times; a block's tile lies in the longitude column of the device that holds the block.
All inputs are finite; a program needn't handle non-finite values.
Results may differ from the reference program's by a relative error of at most 0.0085.
Values may be sent and summed in bfloat16 or wider, within the bound.
A program may use at most 64 MiB of HBM per device.

```python
import math
import jax
import jax.numpy as jnp
from jax import lax

C = 128
TH = 8
TW = 256
OBS = 128
PH = 4
PW = 32
CAP = 2
P_SIZE = 128
NB_DEV = 4
BLOCKS = 32
GRID_LAT = 32
GRID_LON = 512
N_LAT = 4
N_LON = 2


def draw_dest_tile(key, part):
    base = jax.random.fold_in(key, 101)
    key_busiest, key_popular, key_scores, key_reorder = jax.random.split(base, 4)
    sources = N_LAT * N_LON
    entries = N_LAT * CAP
    busiest = jax.random.randint(key_busiest, (), 0, N_LAT)
    popular = jax.random.randint(key_popular, (N_LAT,), 0, 4)
    entry_tile = jnp.arange(entries, dtype=jnp.int32) // CAP
    random_part = jax.random.randint(key_scores, (sources, entries), 0, 65536)
    scores = random_part + popular[entry_tile][None, :] * 16384 + jnp.where(entry_tile == busiest, 1048576, 0)[None, :]
    scores = scores * entries + jnp.arange(entries, dtype=jnp.int32)[None, :]
    picked = lax.top_k(scores, NB_DEV)[1]
    lat_tiles = picked // CAP
    reorder_key = jax.random.randint(key_reorder, (sources, NB_DEV), 0, 65536) * NB_DEV + jnp.arange(NB_DEV, dtype=jnp.int32)[None, :]
    reorder = jnp.argsort(reorder_key, axis=1, stable=True)
    return jnp.take_along_axis(lat_tiles, reorder, axis=1).reshape(-1).astype(jnp.int32)


def place_ends(drawn, stream_key, least, largest):
    longest = drawn.shape.index(max(drawn.shape))
    spots = []
    for shift in (0, 1):
        where = [jax.random.randint(jax.random.fold_in(stream_key, axis), (), 0, length) for axis, length in enumerate(drawn.shape)]
        where[longest] = (where[longest] + shift) % drawn.shape[longest]
        spots.append(tuple(where))
    return drawn.at[spots[0]].set(least).at[spots[1]].set(largest)


def steps_of(key, extent, shards, low, top_value):
    level, own = 1.0, jax.random.fold_in(key, 6)
    for axis_at, shards_of in shards:
        draws = jnp.exp(jax.random.uniform(jax.random.fold_in(own, axis_at), (shards_of,), jnp.float32, low / len(shards), top_value / len(shards)))
        level = level * jnp.repeat(draws, extent[axis_at] // shards_of).reshape([-1 if axis == axis_at else 1 for axis in range(len(extent))])
    return level


def gaussian(rng, extent, deviation, most, cuts=(), held_as=jnp.bfloat16):
    result = jax.random.normal(rng, extent, jnp.float32) * deviation
    if len(cuts) > 0:
        result = steps_of(rng, extent, cuts, -0.22, 0.18) * result
    return jnp.clip(result, min=-most, max=most).astype(held_as)


def setup_inputs(seed: int = 0, part: int = 0) -> dict:
    splits = jax.random.split(jax.random.key(seed), 11)
    own_keys = jax.random.split(jax.random.fold_in(splits[10], part), 11)
    noisy_state = gaussian(own_keys[0], (C, GRID_LAT, GRID_LON), 1.0, 6.0, ((0, 2), (1, 4), (2, 2)))
    kernel_in = gaussian(splits[1], (3, 3, C, C), (9 * C) ** -0.5, 0.1875)
    bias_in = gaussian(splits[2], (C,), 1.0, 4.0, (), jnp.float32)
    kernel_out = gaussian(splits[3], (3, 3, C, C), (9 * C) ** -0.5, 0.1875)
    interp_weight = gaussian(own_keys[4], (BLOCKS, OBS, P_SIZE), P_SIZE ** -0.5, 0.5, ((0, 8),))
    observed = gaussian(own_keys[5], (BLOCKS, C, OBS), 1.0, 6.0, ((0, 8), (1, 2)))
    obs_precision = jnp.clip(jnp.exp(math.log(3.0) - 2.306499 * jax.random.uniform(own_keys[6], (BLOCKS, OBS), jnp.float32) ** steps_of(own_keys[6], (BLOCKS, OBS), ((0, 8),), -0.2, 0.2)), 0.29882812, 3.0).astype(jnp.bfloat16)
    dest_tile = draw_dest_tile(jax.random.fold_in(jax.random.fold_in(splits[10], part), 71), part)
    row_offset = place_ends(jax.random.randint(own_keys[8], (BLOCKS,), 0, TH - PH + 1), jax.random.fold_in(own_keys[8], 1), 0, TH - PH).astype(jnp.int32)
    col_offset = place_ends(jax.random.randint(own_keys[9], (BLOCKS,), 0, TW - PW + 1), jax.random.fold_in(own_keys[9], 1), 0, TW - PW).astype(jnp.int32)
    return {"noisy_state": noisy_state, "kernel_in": kernel_in, "bias_in": bias_in, "kernel_out": kernel_out, "interp_weight": interp_weight, "observed": observed, "obs_precision": obs_precision, "dest_tile": dest_tile, "row_offset": row_offset, "col_offset": col_offset}


def pad_field(grid_field):
    taller = jnp.pad(grid_field, ((0, 0), (1, 1), (0, 0)))
    return jnp.concatenate([taller[:, :, -1:], taller, taller[:, :, :1]], axis=2)


def convolve(grid_field, kernel):
    padded = pad_field(grid_field)
    channels, grid_rows, grid_cols = grid_field.shape
    summed = jnp.zeros((kernel.shape[2], grid_rows * grid_cols), jnp.float32)
    for tap_row in range(3):
        for tap_col in range(3):
            window = padded[:, tap_row:tap_row + grid_rows, tap_col:tap_col + grid_cols].reshape(channels, grid_rows * grid_cols)
            summed = summed + jnp.dot(kernel[tap_row, tap_col], window, preferred_element_type=jnp.float32)
    return summed.reshape(kernel.shape[2], grid_rows, grid_cols)


def adjoint_kernel(kernel):
    return jnp.transpose(kernel[::-1, ::-1], (0, 1, 3, 2))


def extract(grid_field, patch_rows, patch_cols):
    def take_one(row_start, col_start):
        return lax.dynamic_slice(grid_field, (jnp.zeros((), jnp.int32), row_start, col_start), (grid_field.shape[0], PH, PW))
    return jax.vmap(take_one)(patch_rows, patch_cols)


def spread(grad_patch, patch_rows, patch_cols, grid_shape):
    cell_rows = patch_rows[:, None, None] + lax.broadcasted_iota(jnp.int32, (1, PH, 1), 1)
    cell_cols = patch_cols[:, None, None] + lax.broadcasted_iota(jnp.int32, (1, 1, PW), 2)
    return jnp.zeros(grid_shape, jnp.float32).at[:, cell_rows, cell_cols].add(jnp.moveaxis(grad_patch, 1, 0))


def reference(noisy_state, kernel_in, bias_in, kernel_out, interp_weight, observed, obs_precision, dest_tile, row_offset, col_offset):
    pre_act = convolve(noisy_state, kernel_in) + bias_in[:, None, None]
    hidden = jax.nn.silu(pre_act).astype(jnp.bfloat16)
    denoised = (noisy_state.astype(jnp.float32) + convolve(hidden, kernel_out)).astype(jnp.bfloat16)
    blocks = dest_tile.shape[0]
    device_of = jnp.arange(blocks, dtype=jnp.int32) // NB_DEV
    patch_rows = (dest_tile * TH + row_offset).astype(jnp.int32)
    patch_cols = ((device_of % N_LON) * TW + col_offset).astype(jnp.int32)
    patches = extract(denoised, patch_rows, patch_cols).reshape(blocks, noisy_state.shape[0], PH * PW)
    predicted = jnp.einsum("scp,sop->sco", patches.astype(jnp.float32), interp_weight.astype(jnp.float32))
    residual = predicted - observed.astype(jnp.float32)
    innovation = residual.astype(jnp.bfloat16)
    weighted = (residual * obs_precision.astype(jnp.float32)[:, None, :]).astype(jnp.bfloat16)
    pulled = jnp.einsum("sco,sop->scp", weighted.astype(jnp.float32), interp_weight.astype(jnp.float32))
    grad_field = spread(pulled.reshape(blocks, noisy_state.shape[0], PH, PW), patch_rows, patch_cols, noisy_state.shape)
    grad_round = grad_field.astype(jnp.bfloat16)
    back_hidden = convolve(grad_round, adjoint_kernel(kernel_out))
    sigmoid_act = jax.nn.sigmoid(pre_act)
    grad_pre = (back_hidden * sigmoid_act * (1.0 + pre_act * (1.0 - sigmoid_act))).astype(jnp.bfloat16)
    grad_state = grad_field + convolve(grad_pre, adjoint_kernel(kernel_in))
    next_state = 0.6 * noisy_state.astype(jnp.float32) + 0.4 * denoised.astype(jnp.float32) - 0.3 * grad_state
    return next_state, innovation
```

```python
import functools

import jax
import jax.numpy as jnp
from jax import lax
from jax.experimental import pallas as pl
from jax.experimental.pallas import tpu as pltpu
from jax.sharding import PartitionSpec as P

PH = 4
PW = 32
CAP = 2
HALO = 2
SIDE = 16
META = 16

keep_rate = 0.6
blend_rate = 0.4
guide_rate = 0.3

MESH = pl.DeviceIdType.MESH
F32 = jnp.float32
BF16 = jnp.bfloat16


def kernel(
    n_lat, n_lon, rows, width, half, blocks,
    dest, row_off, col_off, x, kfi, kfo, kao, kai, bias, weight, values, scale,
    out, inn_out,
    both, X, X3, pre, base, D, E, pay, R, G, GF, inn, inn_r, out_s, out_r, pulled_s,
    plan,
    halo_s, halo_r, pair_s, pair_r, pay_s, pay_r, inn_ss, inn_rs,
):
    lat, lon, ch = lax.axis_index("lat"), lax.axis_index("lon"), lax.axis_index("ch")
    other = 1 - ch
    chans = 2 * half
    obs = weight.shape[1]
    cells = PH * PW
    pitch = width + 2 * SIDE
    slots = n_lat * CAP
    px = rows * width
    lon_right = lax.rem(lon + ch, n_lon)
    lon_left = lax.rem(lon + n_lon - other, n_lon)
    has_up = lat > 0
    has_down = lat < n_lat - 1
    sibling = {"ch": other}

    def at(dlat, side):
        place = {"lat": lat + dlat}
        if side:
            place["lon"] = lon_right if side > 0 else lon_left
            place["ch"] = other
        return place

    barrier = pltpu.get_barrier_semaphore()

    def greet(place):
        pl.semaphore_signal(barrier, inc=1, device_id=place, device_id_type=MESH)

    for step in range(1, n_lat):
        greet({"lat": lax.rem(lat + step, n_lat)})
    greet(at(0, -1))
    greet(at(0, 1))

    @pl.when(has_up)
    def _():
        greet(at(-1, -1))
        greet(at(-1, 1))

    @pl.when(has_down)
    def _():
        greet(at(1, -1))
        greet(at(1, 1))

    def count_block(b, _):
        def earlier(e, rank):
            return rank + jnp.where(dest[e] == dest[b], 1, 0)

        plan[b] = dest[b] * CAP + lax.fori_loop(0, b, earlier, 0)
        return 0

    for b in range(blocks) if blocks <= 8 else ():
        rank = 0
        for e in range(b):
            rank = rank + jnp.where(dest[e] == dest[b], 1, 0)
        plan[b] = dest[b] * CAP + rank
    if blocks > 8:
        lax.fori_loop(0, blocks, count_block, 0)

    def pack_slot(s, _):
        def look(b, found):
            return jnp.where(plan[b] == s, b, found)

        found = lax.fori_loop(0, blocks, look, -1)
        source = jnp.maximum(found, 0)
        fill = jnp.where(found >= 0, 1.0, 0.0)
        w = (weight[source].astype(F32) * fill).astype(BF16)
        t = s // CAP
        k = s % CAP
        pay[t, k, 0:half] = w_half(w)
        pay[t, k, half:chans] = values[source]
        level = lax.broadcasted_iota(jnp.int32, (META, obs), 0)
        r0 = row_off[source].astype(F32)
        q0 = col_off[source].astype(F32)
        meta = jnp.where(level == 0, scale[source], jnp.where(level == 1, r0, q0))
        pay[t, k, chans : chans + META] = meta.astype(BF16)
        return 0

    def w_half(w):
        return jnp.where(ch == 0, w[0:half].astype(F32), w[half:chans].astype(F32)).astype(BF16)

    lax.fori_loop(0, slots, pack_slot, 0)

    tops = (lat + n_lat - 1) // n_lat
    bottoms = (2 * n_lat - 2 - lat) // n_lat
    pl.semaphore_wait(barrier, n_lat + 1 + 2 * tops + 2 * bottoms)

    def pair_copy(src, dst, i):
        return pltpu.make_async_remote_copy(
            src_ref=src, dst_ref=dst, send_sem=pair_s.at[i], recv_sem=pair_r.at[i],
            device_id=sibling, device_id_type=MESH,
        )

    reshard = pair_copy(x.at[other], both.at[ch], 0)
    reshard.start()
    both[ch] = x[ch]

    top, left = HALO, SIDE
    spans_r = {-1: (top, 0 + rows + top), 0: (top, top), 1: (top + rows - HALO, 0)}
    spans_c = {-1: (left, left + width), 0: (left, left), 1: (left + width - SIDE, 0)}
    size_r = {-1: HALO, 0: rows, 1: HALO}
    size_c = {-1: SIDE, 0: width, 1: SIDE}
    routes = [(0, -1), (0, 1), (-1, 0), (-1, -1), (-1, 1), (1, 0), (1, -1), (1, 1)]

    def halo_copy(buf, i, base_sem):
        dl, side = routes[i]
        sr, dr = spans_r[dl]
        sc, dc = spans_c[side]
        src = buf.at[pl.ds(sr, size_r[dl]), pl.ds(sc, size_c[side])]
        dst = buf.at[pl.ds(dr, size_r[dl]), pl.ds(dc, size_c[side])]
        return pltpu.make_async_remote_copy(
            src_ref=src, dst_ref=dst,
            send_sem=halo_s.at[base_sem + i], recv_sem=halo_r.at[base_sem + i],
            device_id=at(dl, side), device_id_type=MESH,
        )

    def halo_wait_recv(buf, i, base_sem):
        halo_copy(buf, i, base_sem).wait_recv()

    def guarded(dl, fn):
        if dl == 0:
            fn()
        else:
            pl.when(has_up if dl < 0 else has_down)(fn)

    def halo_start(buf, base_sem):
        for dl in (-1, 1, 0):
            def go(dl=dl):
                for i, route in enumerate(routes):
                    if route[0] == dl:
                        halo_copy(buf, i, base_sem).start()

            guarded(dl, go)

    def halo_finish(buf, base_sem):
        for dl in (0, -1, 1):
            def go(dl=dl):
                for i, route in enumerate(routes):
                    if route[0] == dl:
                        halo_copy(buf, i, base_sem).wait_send()

            def got(dl=dl):
                for i, route in enumerate(routes):
                    if route[0] == dl:
                        halo_wait_recv(buf, i, base_sem)

            guarded(dl, go)
            guarded(-dl, got)

    def clear_poles(buf):
        @pl.when(lat == 0)
        def _():
            buf[0:HALO] = jnp.zeros((HALO, pitch, chans), BF16)

        @pl.when(lat == n_lat - 1)
        def _():
            buf[rows + HALO : rows + 2 * HALO] = jnp.zeros((HALO, pitch, chans), BF16)

    def put_row(r, v):
        X3[r * pitch : (r + 1) * pitch, 0:chans] = pltpu.roll(v, 1, 0).astype(BF16)
        X3[r * pitch : (r + 1) * pitch, chans : 2 * chans] = v.astype(BF16)
        X3[r * pitch : (r + 1) * pitch, 2 * chans :] = pltpu.roll(v, pitch - 1, 0).astype(BF16)

    def conv(kmat, first, count):
        acc = None
        for a in range(3):
            part = jnp.dot(
                X3[(first + a) * pitch : (first + a + count) * pitch, :], kmat[a],
                preferred_element_type=F32,
            )
            acc = part if acc is None else acc + part
        return acc

    def edge_factor(r):
        if r == 0:
            return jnp.where(has_up, 1.0, 0.0)
        if r == rows + 1:
            return jnp.where(has_down, 1.0, 0.0)
        return None

    clear_poles(X)
    clear_poles(G)

    reshard.wait()
    for r in range(rows):
        X[top + r, left : left + width] = jnp.concatenate([both[0, r], both[1, r]], axis=-1)
    halo_start(X, 0)

    def pay_copy(i, step):
        peer = lax.rem(lat + step, n_lat)
        return pltpu.make_async_remote_copy(
            src_ref=pay.at[peer], dst_ref=R.at[lat, ch],
            send_sem=pay_s.at[i], recv_sem=pay_r.at[i],
            device_id={"lat": peer}, device_id_type=MESH,
        )

    for step in range(1, n_lat):
        pay_copy(step - 1, step).start()
    R[lat, ch] = pay[lat]

    halo_finish(X, 0)
    for r in range(rows + 2 * HALO):
        put_row(r, X[r].astype(F32))

    CH = 2
    for r0 in range(0, rows + 2, CH):
        acc = conv(kfi, r0, CH) + bias[...]
        pre[r0 * pitch : (r0 + CH) * pitch, :] = acc
    for r in range(rows + 2):
        v = pre[r * pitch : (r + 1) * pitch, :]
        h = v / (1.0 + jnp.exp(-v))
        f = edge_factor(r)
        if f is not None:
            h = h * f
        put_row(r, h.astype(BF16).astype(F32))

    for step in range(1, n_lat):
        pay_copy(step - 1, step).wait()
    forward = pair_copy(R.at[:, ch], R.at[:, ch], 1)
    forward.start()

    for r0 in range(0, rows, CH):
        acc = conv(kfo, r0, CH)
        for i in range(CH):
            r = r0 + i
            state = X[top + r, left : left + width].astype(F32)
            den = (state + acc[i * pitch + left : i * pitch + left + width]).astype(BF16)
            base[r * width : (r + 1) * width, :] = keep_rate * state + blend_rate * den.astype(F32)
            D[ch, :, r * width : (r + 1) * width] = den.astype(F32).T.astype(BF16)
    swap = pair_copy(D.at[ch], D.at[ch], 2)
    swap.start()

    forward.wait()
    lane = lax.broadcasted_iota(jnp.int32, (1, cells), 1)
    cell_r = (lane // PW).astype(F32)
    cell_c = (lane % PW).astype(F32)

    def place_slot(s, _):
        t = s // CAP
        k = s % CAP
        meta = R[t, 0, k, chans : chans + META].astype(F32)
        q = meta[2:3] + cell_c
        target = (meta[1:2] + cell_r) * width + q + jnp.where(q >= width, float(px - width), 0.0)
        index = lax.broadcasted_iota(jnp.int32, (2 * px, cells), 0).astype(F32)
        E[s] = jnp.where(index == target, 1.0, 0.0).astype(BF16)
        return 0

    lax.fori_loop(0, slots, place_slot, 0)
    swap.wait()

    def observe_slot(s, _):
        t = s // CAP
        k = s % CAP
        patch = jnp.dot(D[0], E[s, 0:px], preferred_element_type=F32) + jnp.dot(
            D[1], E[s, px : 2 * px], preferred_element_type=F32
        )
        w = jnp.concatenate([R[t, 0, k, 0:half], R[t, 1, k, 0:half]], axis=0)
        val = jnp.concatenate([R[t, 0, k, half:chans], R[t, 1, k, half:chans]], axis=0)
        predicted = lax.dot_general(
            patch.astype(BF16), w, (((1,), (1,)), ((), ())), preferred_element_type=F32
        )
        residual = predicted - val.astype(F32)
        inn[t, k] = jnp.where(ch == 0, residual[0:half], residual[half:chans]).astype(BF16)
        sc = R[t, 0, k, chans : chans + META].astype(F32)[0:1]
        weighted = (residual * sc).astype(BF16)
        pulled_s[s] = jnp.dot(weighted, w, preferred_element_type=F32).astype(BF16)
        return 0

    lax.fori_loop(0, slots, observe_slot, 0)

    GF[...] = jnp.zeros((px, chans), F32)

    def spread_slot(s, _):
        GF[...] += lax.dot_general(
            E[s, pl.ds(pl.multiple_of(ch * px, px), px)], pulled_s[s],
            (((1,), (1,)), ((), ())), preferred_element_type=F32,
        )
        return 0

    lax.fori_loop(0, slots, spread_slot, 0)
    for r in range(rows):
        G[top + r, left : left + width] = GF[r * width : (r + 1) * width, :].astype(BF16)
    halo_start(G, 8)

    def inn_copy(i, step):
        peer = lax.rem(lat + step, n_lat)
        return pltpu.make_async_remote_copy(
            src_ref=inn.at[peer], dst_ref=inn_r.at[lat],
            send_sem=inn_ss.at[i], recv_sem=inn_rs.at[i],
            device_id={"lat": peer}, device_id_type=MESH,
        )

    for step in range(1, n_lat):
        inn_copy(step - 1, step).start()
    inn_r[lat] = inn[lat]
    halo_finish(G, 8)
    for r in range(rows + 2 * HALO):
        put_row(r, G[r].astype(F32))
    for r0 in range(0, rows + 2, CH):
        part = slice(r0 * pitch, (r0 + CH) * pitch)
        back = conv(kao, r0, CH)
        v = pre[part, :]
        s = 1.0 / (1.0 + jnp.exp(-v))
        pre[part, :] = back * s * (1.0 + v * (1.0 - s))
    for r in range(rows + 2):
        g = pre[r * pitch : (r + 1) * pitch, :]
        f = edge_factor(r)
        if f is not None:
            g = g * f
        put_row(r, g.astype(BF16).astype(F32))
    for r0 in range(0, rows, CH):
        acc = conv(kai, r0, CH)
        for i in range(CH):
            r = r0 + i
            own = slice(r * width, (r + 1) * width)
            grad = GF[own, :] + acc[i * pitch + left : i * pitch + left + width]
            res = (base[own, :] - guide_rate * grad).T
            out_s[0, :, own] = res[0:half]
            out_s[1, :, own] = res[half:chans]
    back_home = pair_copy(out_s.at[other], out_r, 3)
    back_home.start()
    out[ch] = out_s[ch]
    for step in range(1, n_lat):
        inn_copy(step - 1, step).wait()

    def fetch(b, _):
        slot = plan[b]
        inn_out[b] = inn_r[slot // CAP, slot % CAP]
        return 0

    lax.fori_loop(0, blocks, fetch, 0)
    back_home.wait()
    out[other] = out_r[...]


def body(n_lat, n_lon, noisy_state, kernel_in, bias_in, kernel_out, interp_weight, observed,
         obs_precision, dest_tile, row_offset, col_offset):
    half, rows, cols = noisy_state.shape
    chans = 2 * half
    width = cols // 2
    blocks, obs, cells = interp_weight.shape
    slots = n_lat * CAP
    pitch = width + 2 * SIDE
    px = rows * width
    x = jnp.transpose(noisy_state.reshape(half, rows, 2, width), (2, 1, 3, 0))

    def forward(k):
        return jnp.transpose(k, (0, 1, 3, 2)).reshape(3, 3 * chans, chans)

    def adjoint(k):
        return k[::-1, ::-1].reshape(3, 3 * chans, chans)

    vmem = pl.BlockSpec(memory_space=pltpu.VMEM)
    smem = pl.BlockSpec(memory_space=pltpu.SMEM)
    call = pl.pallas_call(
        functools.partial(kernel, n_lat, n_lon, rows, width, half, blocks),
        out_shape=(
            jax.ShapeDtypeStruct((2, half, px), F32),
            jax.ShapeDtypeStruct((blocks, half, obs), BF16),
        ),
        in_specs=[smem] * 3 + [vmem] * 9,
        out_specs=(vmem, vmem),
        scratch_shapes=[
            pltpu.VMEM((2, rows, width, half), BF16),
            pltpu.VMEM((rows + 4, pitch, chans), BF16),
            pltpu.VMEM(((rows + 4) * pitch, 3 * chans), BF16),
            pltpu.VMEM(((rows + 2) * pitch, chans), F32),
            pltpu.VMEM((px, chans), F32),
            pltpu.VMEM((2, chans, px), BF16),
            pltpu.VMEM((slots, 2 * px, cells), BF16),
            pltpu.VMEM((n_lat, CAP, chans + META, obs), BF16),
            pltpu.VMEM((n_lat, 2, CAP, chans + META, obs), BF16),
            pltpu.VMEM((rows + 4, pitch, chans), BF16),
            pltpu.VMEM((px, chans), F32),
            pltpu.VMEM((n_lat, CAP, half, obs), BF16),
            pltpu.VMEM((n_lat, CAP, half, obs), BF16),
            pltpu.VMEM((2, half, px), F32),
            pltpu.VMEM((half, px), F32),
            pltpu.VMEM((slots, chans, cells), BF16),
            pltpu.SMEM((blocks,), jnp.int32),
            pltpu.SemaphoreType.DMA((16,)),
            pltpu.SemaphoreType.DMA((16,)),
            pltpu.SemaphoreType.DMA((4,)),
            pltpu.SemaphoreType.DMA((4,)),
            pltpu.SemaphoreType.DMA((n_lat - 1,)),
            pltpu.SemaphoreType.DMA((n_lat - 1,)),
            pltpu.SemaphoreType.DMA((n_lat - 1,)),
            pltpu.SemaphoreType.DMA((n_lat - 1,)),
        ],
        compiler_params=pltpu.CompilerParams(
            collective_id=0, has_side_effects=True, vmem_limit_bytes=63 * 1024 * 1024
        ),
    )
    out, innovation = call(
        dest_tile, row_offset, col_offset, x,
        forward(kernel_in), forward(kernel_out), adjoint(kernel_out), adjoint(kernel_in),
        bias_in.reshape(1, chans), interp_weight, observed,
        obs_precision.astype(F32).reshape(blocks, 1, obs),
    )
    next_state = jnp.transpose(out.reshape(2, half, rows, width), (1, 2, 0, 3))
    return next_state.reshape(half, rows, cols), innovation


def solution(mesh):
    return jax.shard_map(
        functools.partial(body, mesh.shape["lat"], mesh.shape["lon"]),
        mesh=mesh,
        in_specs=(
            P(("grp", "ch"), "lat", "lon"),
            P(),
            P(),
            P(),
            P(("grp", "lat", "lon"), None, None),
            P(("grp", "lat", "lon"), "ch", None),
            P(("grp", "lat", "lon"), None),
            P(("grp", "lat", "lon")),
            P(("grp", "lat", "lon")),
            P(("grp", "lat", "lon")),
        ),
        out_specs=(P(("grp", "ch"), "lat", "lon"), P(("grp", "lat", "lon"), "ch", None)),
        check_vma=False,
    )
```

```python
import functools

import jax
import jax.numpy as jnp
from jax import lax
from jax.experimental import pallas as pl
from jax.experimental.pallas import tpu as pltpu
from jax.sharding import PartitionSpec as P

PH = 4
PW = 32
CAP = 2
HALO = 2
SIDE = 16
META = 16
GROUP = 8

keep_rate = 0.6
blend_rate = 0.4
guide_rate = 0.3

MESH = pl.DeviceIdType.MESH
F32 = jnp.float32
BF16 = jnp.bfloat16


def kernel(
    n_lat, n_lon, rows, width, half, blocks,
    dest, row_off, col_off, x_hbm, kin_hbm, kout_hbm, bias, weight_hbm, values_hbm, scale_hbm,
    out, inn_out,
    xv, xs, x_send, kin, kout, weight, values, scale_raw, scale, kfi, kfo, load_sem,
    both, X, X3, pre, base, D, E, pay, R, G, GF, inn, inn_r, out_s, out_r, pulled_s,
    plan,
    halo_s, halo_r, pair_s, pair_r, pay_s, pay_r, inn_ss, inn_rs,
):
    lat, lon, ch = lax.axis_index("lat"), lax.axis_index("lon"), lax.axis_index("ch")
    other = 1 - ch
    chans = 2 * half
    obs = weight_hbm.shape[1]
    cells = PH * PW
    pitch = width + 2 * SIDE
    slots = n_lat * CAP
    px = rows * width
    lon_right = lax.rem(lon + ch, n_lon)
    lon_left = lax.rem(lon + n_lon - other, n_lon)
    has_up = lat > 0
    has_down = lat < n_lat - 1
    sibling = {"ch": other}

    def at(dlat, side):
        place = {"lat": lat + dlat}
        if side:
            place["lon"] = lon_right if side > 0 else lon_left
            place["ch"] = other
        return place

    loads = [
        pltpu.make_async_copy(src, dst, load_sem.at[i])
        for i, (src, dst) in enumerate(
            [(x_hbm, xv), (weight_hbm, weight), (values_hbm, values), (scale_hbm, scale_raw),
             (kin_hbm, kin), (kout_hbm, kout)]
        )
    ]
    for load in loads:
        load.start()
    barrier = pltpu.get_barrier_semaphore()

    def greet(place):
        pl.semaphore_signal(barrier, inc=1, device_id=place, device_id_type=MESH)

    for step in range(1, n_lat):
        greet({"lat": lax.rem(lat + step, n_lat)})
    greet(at(0, -1))
    greet(at(0, 1))

    @pl.when(has_up)
    def _():
        greet(at(-1, -1))
        greet(at(-1, 1))

    @pl.when(has_down)
    def _():
        greet(at(1, -1))
        greet(at(1, 1))

    def count_block(b, _):
        def earlier(e, rank):
            return rank + jnp.where(dest[e] == dest[b], 1, 0)

        plan[b] = dest[b] * CAP + lax.fori_loop(0, b, earlier, 0)
        return 0

    for b in range(blocks) if blocks <= 8 else ():
        rank = 0
        for e in range(b):
            rank = rank + jnp.where(dest[e] == dest[b], 1, 0)
        plan[b] = dest[b] * CAP + rank
    if blocks > 8:
        lax.fori_loop(0, blocks, count_block, 0)

    def pack_slot(s, _):
        def look(b, found):
            return jnp.where(plan[b] == s, b, found)

        found = lax.fori_loop(0, blocks, look, -1)
        source = jnp.maximum(found, 0)
        fill = jnp.where(found >= 0, 1.0, 0.0)
        w = (weight[source].astype(F32) * fill).astype(BF16)
        t = s // CAP
        k = s % CAP
        pay[t, k, 0:half] = w_half(w)
        pay[t, k, half:chans] = values[source]
        level = lax.broadcasted_iota(jnp.int32, (META, obs), 0)
        r0 = row_off[source].astype(F32)
        q0 = col_off[source].astype(F32)
        meta = jnp.where(level == 0, scale[pl.ds(source, 1), :], jnp.where(level == 1, r0, q0))
        pay[t, k, chans : chans + META] = meta.astype(BF16)
        return 0

    def w_half(w):
        return jnp.where(ch == 0, w[0:half].astype(F32), w[half:chans].astype(F32)).astype(BF16)

    loads[0].wait()
    for h in range(2):
        part = xv[:, :, h * width : (h + 1) * width].astype(F32)
        xs[h] = part.reshape(half * rows, width)
    for r in range(rows):
        both[ch, r] = xs[ch, pl.ds(r, half, stride=rows), :].astype(BF16)
        x_send[r] = xs[other, pl.ds(r, half, stride=rows), :].astype(BF16)

    tops = (lat + n_lat - 1) // n_lat
    bottoms = (2 * n_lat - 2 - lat) // n_lat
    pl.semaphore_wait(barrier, n_lat + 1 + 2 * tops + 2 * bottoms)

    def pair_copy(src, dst, i):
        return pltpu.make_async_remote_copy(
            src_ref=src, dst_ref=dst, send_sem=pair_s.at[i], recv_sem=pair_r.at[i],
            device_id=sibling, device_id_type=MESH,
        )

    reshard = pair_copy(x_send, both.at[ch], 0)
    reshard.start()
    for load in loads[1:4]:
        load.wait()
    scale[...] = scale_raw[...].astype(F32)
    lax.fori_loop(0, slots, pack_slot, 0)

    top, left = HALO, SIDE
    spans_r = {-1: (top, 0 + rows + top), 0: (top, top), 1: (top + rows - HALO, 0)}
    spans_c = {-1: (left, left + width), 0: (left, left), 1: (left + width - SIDE, 0)}
    size_r = {-1: HALO, 0: rows, 1: HALO}
    size_c = {-1: SIDE, 0: width, 1: SIDE}
    routes = [(0, -1), (0, 1), (-1, 0), (-1, -1), (-1, 1), (1, 0), (1, -1), (1, 1)]

    def halo_copy(buf, i, base_sem):
        dl, side = routes[i]
        sr, dr = spans_r[dl]
        sc, dc = spans_c[side]
        src = buf.at[pl.ds(sr, size_r[dl]), pl.ds(sc, size_c[side])]
        dst = buf.at[pl.ds(dr, size_r[dl]), pl.ds(dc, size_c[side])]
        return pltpu.make_async_remote_copy(
            src_ref=src, dst_ref=dst,
            send_sem=halo_s.at[base_sem + i], recv_sem=halo_r.at[base_sem + i],
            device_id=at(dl, side), device_id_type=MESH,
        )

    def halo_wait_recv(buf, i, base_sem):
        halo_copy(buf, i, base_sem).wait_recv()

    def guarded(dl, fn):
        if dl == 0:
            fn()
        else:
            pl.when(has_up if dl < 0 else has_down)(fn)

    def halo_start(buf, base_sem):
        for dl in (-1, 1, 0):
            def go(dl=dl):
                for i, route in enumerate(routes):
                    if route[0] == dl:
                        halo_copy(buf, i, base_sem).start()

            guarded(dl, go)

    def halo_finish(buf, base_sem):
        for dl in (0, -1, 1):
            def go(dl=dl):
                for i, route in enumerate(routes):
                    if route[0] == dl:
                        halo_copy(buf, i, base_sem).wait_send()

            def got(dl=dl):
                for i, route in enumerate(routes):
                    if route[0] == dl:
                        halo_wait_recv(buf, i, base_sem)

            guarded(dl, go)
            guarded(-dl, got)

    def clear_poles(buf):
        @pl.when(lat == 0)
        def _():
            buf[0:HALO] = jnp.zeros((HALO, pitch, chans), BF16)

        @pl.when(lat == n_lat - 1)
        def _():
            buf[rows + HALO : rows + 2 * HALO] = jnp.zeros((HALO, pitch, chans), BF16)

    def put_row(r, v):
        X3[r * pitch : (r + 1) * pitch, 0:chans] = pltpu.roll(v, 1, 0).astype(BF16)
        X3[r * pitch : (r + 1) * pitch, chans : 2 * chans] = v.astype(BF16)
        X3[r * pitch : (r + 1) * pitch, 2 * chans :] = pltpu.roll(v, pitch - 1, 0).astype(BF16)

    def conv(kmat, first, count):
        acc = None
        for a in range(3):
            part = jnp.dot(
                X3[(first + a) * pitch : (first + a + count) * pitch, :], kmat(a),
                preferred_element_type=F32,
            )
            acc = part if acc is None else acc + part
        return acc

    def mirrored(k, a):
        return jnp.concatenate([k[2 - a, 2], k[2 - a, 1], k[2 - a, 0]], axis=0)

    def edge_factor(r):
        if r == 0:
            return jnp.where(has_up, 1.0, 0.0)
        if r == rows + 1:
            return jnp.where(has_down, 1.0, 0.0)
        return None

    clear_poles(X)
    clear_poles(G)

    reshard.wait()
    for r in range(rows):
        X[top + r, left : left + width] = (
            jnp.concatenate([both[0, r], both[1, r]], axis=0).astype(F32).T.astype(BF16)
        )
    halo_start(X, 0)

    def pay_copy(i, step):
        peer = lax.rem(lat + step, n_lat)
        return pltpu.make_async_remote_copy(
            src_ref=pay.at[peer], dst_ref=R.at[lat, ch],
            send_sem=pay_s.at[i], recv_sem=pay_r.at[i],
            device_id={"lat": peer}, device_id_type=MESH,
        )

    for step in range(1, n_lat):
        pay_copy(step - 1, step).start()
    R[lat, ch] = pay[lat]
    for load in loads[4:]:
        load.wait()
    for a in range(3):
        for b in range(3):
            kfi[a, b * chans : (b + 1) * chans] = kin[a, b].astype(F32).T.astype(BF16)
            kfo[a, b * chans : (b + 1) * chans] = kout[a, b].astype(F32).T.astype(BF16)

    halo_finish(X, 0)
    for r in range(rows + 2 * HALO):
        put_row(r, X[r].astype(F32))

    CH = 2
    for r0 in range(0, rows + 2, CH):
        acc = conv(lambda a: kfi[a], r0, CH) + bias[...]
        pre[r0 * pitch : (r0 + CH) * pitch, :] = acc
    for r in range(rows + 2):
        v = pre[r * pitch : (r + 1) * pitch, :]
        h = v / (1.0 + jnp.exp(-v))
        f = edge_factor(r)
        if f is not None:
            h = h * f
        put_row(r, h.astype(BF16).astype(F32))

    for step in range(1, n_lat):
        pay_copy(step - 1, step).wait()
    forward = pair_copy(R.at[:, ch], R.at[:, ch], 1)
    forward.start()

    for r0 in range(0, rows, CH):
        acc = conv(lambda a: kfo[a], r0, CH)
        for i in range(CH):
            r = r0 + i
            state = X[top + r, left : left + width].astype(F32)
            den = (state + acc[i * pitch + left : i * pitch + left + width]).astype(BF16)
            base[r * width : (r + 1) * width, :] = keep_rate * state + blend_rate * den.astype(F32)
            D[ch, :, r * width : (r + 1) * width] = den.astype(F32).T.astype(BF16)
    swap = pair_copy(D.at[ch], D.at[ch], 2)
    swap.start()

    forward.wait()
    lane = lax.broadcasted_iota(jnp.int32, (1, cells), 1)
    cell_r = (lane // PW).astype(F32)
    cell_c = (lane % PW).astype(F32)

    def each_group(fn):
        if slots == GROUP:
            fn(0)
        else:
            lax.fori_loop(0, slots // GROUP, lambda g, _: fn(g) or 0, 0)

    def place_group(g):
        def place_rows(n, _):
            index = lax.broadcasted_iota(jnp.int32, (width, cells), 0) + n * width
            index = index.astype(F32)
            for i in range(GROUP):
                s = g * GROUP + i
                meta = R[s // CAP, 0, s % CAP, chans : chans + META].astype(F32)
                q = meta[2:3] + cell_c
                target = (meta[1:2] + cell_r) * width + q
                target = target + jnp.where(q >= width, float(px - width), 0.0)
                E[g, pl.ds(pl.multiple_of(n * width, width), width), i * cells : (i + 1) * cells] = (
                    jnp.where(index == target, 1.0, 0.0).astype(BF16)
                )
            return 0

        lax.fori_loop(0, 2 * rows, place_rows, 0)

    each_group(place_group)
    swap.wait()

    def observe_group(g):
        patches = jnp.dot(D[0], E[g, 0:px], preferred_element_type=F32) + jnp.dot(
            D[1], E[g, px : 2 * px], preferred_element_type=F32
        )
        patches = patches.astype(BF16)
        for i in range(GROUP):
            s = g * GROUP + i
            t = s // CAP
            k = s % CAP
            own = slice(i * cells, (i + 1) * cells)
            w = jnp.concatenate([R[t, 0, k, 0:half], R[t, 1, k, 0:half]], axis=0)
            val = jnp.concatenate([R[t, 0, k, half:chans], R[t, 1, k, half:chans]], axis=0)
            predicted = lax.dot_general(
                patches[:, own], w, (((1,), (1,)), ((), ())), preferred_element_type=F32
            )
            residual = predicted - val.astype(F32)
            inn[t, k] = jnp.where(ch == 0, residual[0:half], residual[half:chans]).astype(BF16)
            sc = R[t, 0, k, chans : chans + META].astype(F32)[0:1]
            weighted = (residual * sc).astype(BF16)
            pulled_s[g, :, own] = jnp.dot(weighted, w, preferred_element_type=F32).astype(BF16)

    each_group(observe_group)

    def spread_group(g):
        added = lax.dot_general(
            E[g, pl.ds(pl.multiple_of(ch * px, px), px)], pulled_s[g],
            (((1,), (1,)), ((), ())), preferred_element_type=F32,
        )
        if slots == GROUP:
            GF[...] = added
        else:
            GF[...] += added

    if slots != GROUP:
        GF[...] = jnp.zeros((px, chans), F32)
    each_group(spread_group)
    for r in range(rows):
        G[top + r, left : left + width] = GF[r * width : (r + 1) * width, :].astype(BF16)
    halo_start(G, 8)

    def inn_copy(i, step):
        peer = lax.rem(lat + step, n_lat)
        return pltpu.make_async_remote_copy(
            src_ref=inn.at[peer], dst_ref=inn_r.at[lat],
            send_sem=inn_ss.at[i], recv_sem=inn_rs.at[i],
            device_id={"lat": peer}, device_id_type=MESH,
        )

    for step in range(1, n_lat):
        inn_copy(step - 1, step).start()
    inn_r[lat] = inn[lat]
    halo_finish(G, 8)
    for r in range(rows + 2 * HALO):
        put_row(r, G[r].astype(F32))
    for r0 in range(0, rows + 2, CH):
        part = slice(r0 * pitch, (r0 + CH) * pitch)
        back = conv(lambda a: mirrored(kout, a), r0, CH)
        v = pre[part, :]
        s = 1.0 / (1.0 + jnp.exp(-v))
        pre[part, :] = back * s * (1.0 + v * (1.0 - s))
    for r in range(rows + 2):
        g = pre[r * pitch : (r + 1) * pitch, :]
        f = edge_factor(r)
        if f is not None:
            g = g * f
        put_row(r, g.astype(BF16).astype(F32))
    for r0 in range(0, rows, CH):
        acc = conv(lambda a: mirrored(kin, a), r0, CH)
        for i in range(CH):
            r = r0 + i
            own = slice(r * width, (r + 1) * width)
            grad = GF[own, :] + acc[i * pitch + left : i * pitch + left + width]
            res = (base[own, :] - guide_rate * grad).T
            out_s[0, pl.ds(r, half, stride=rows), :] = res[0:half]
            out_s[1, pl.ds(r, half, stride=rows), :] = res[half:chans]
    back_home = pair_copy(out_s.at[other], out_r, 3)
    back_home.start()
    out[ch] = out_s[ch]
    for step in range(1, n_lat):
        inn_copy(step - 1, step).wait()

    def fetch(b, _):
        slot = plan[b]
        inn_out[b] = inn_r[slot // CAP, slot % CAP]
        return 0

    lax.fori_loop(0, blocks, fetch, 0)
    back_home.wait()
    out[other] = out_r[...]


def body(n_lat, n_lon, noisy_state, kernel_in, bias_in, kernel_out, interp_weight, observed,
         obs_precision, dest_tile, row_offset, col_offset):
    half, rows, cols = noisy_state.shape
    chans = 2 * half
    width = cols // 2
    blocks, obs, cells = interp_weight.shape
    slots = n_lat * CAP
    pitch = width + 2 * SIDE
    px = rows * width
    vmem = pl.BlockSpec(memory_space=pltpu.VMEM)
    hbm = pl.BlockSpec(memory_space=pl.ANY)
    smem = pl.BlockSpec(memory_space=pltpu.SMEM)
    call = pl.pallas_call(
        functools.partial(kernel, n_lat, n_lon, rows, width, half, blocks),
        out_shape=(
            jax.ShapeDtypeStruct((2, half * rows, width), F32),
            jax.ShapeDtypeStruct((blocks, half, obs), BF16),
        ),
        in_specs=[smem] * 3 + [hbm] * 3 + [vmem] + [hbm] * 3,
        out_specs=(vmem, vmem),
        scratch_shapes=[
            pltpu.VMEM((half, rows, cols), BF16),
            pltpu.VMEM((2, half * rows, width), F32),
            pltpu.VMEM((rows, half, width), BF16),
            pltpu.VMEM(kernel_in.shape, BF16),
            pltpu.VMEM(kernel_out.shape, BF16),
            pltpu.VMEM(interp_weight.shape, BF16),
            pltpu.VMEM(observed.shape, BF16),
            pltpu.VMEM(obs_precision.shape, BF16),
            pltpu.VMEM(obs_precision.shape, F32),
            pltpu.VMEM((3, 3 * chans, chans), BF16),
            pltpu.VMEM((3, 3 * chans, chans), BF16),
            pltpu.SemaphoreType.DMA((6,)),
            pltpu.VMEM((2, rows, half, width), BF16),
            pltpu.VMEM((rows + 4, pitch, chans), BF16),
            pltpu.VMEM(((rows + 4) * pitch, 3 * chans), BF16),
            pltpu.VMEM(((rows + 2) * pitch, chans), F32),
            pltpu.VMEM((px, chans), F32),
            pltpu.VMEM((2, chans, px), BF16),
            pltpu.VMEM((slots // GROUP, 2 * px, GROUP * cells), BF16),
            pltpu.VMEM((n_lat, CAP, chans + META, obs), BF16),
            pltpu.VMEM((n_lat, 2, CAP, chans + META, obs), BF16),
            pltpu.VMEM((rows + 4, pitch, chans), BF16),
            pltpu.VMEM((px, chans), F32),
            pltpu.VMEM((n_lat, CAP, half, obs), BF16),
            pltpu.VMEM((n_lat, CAP, half, obs), BF16),
            pltpu.VMEM((2, half * rows, width), F32),
            pltpu.VMEM((half * rows, width), F32),
            pltpu.VMEM((slots // GROUP, chans, GROUP * cells), BF16),
            pltpu.SMEM((blocks,), jnp.int32),
            pltpu.SemaphoreType.DMA((16,)),
            pltpu.SemaphoreType.DMA((16,)),
            pltpu.SemaphoreType.DMA((4,)),
            pltpu.SemaphoreType.DMA((4,)),
            pltpu.SemaphoreType.DMA((n_lat - 1,)),
            pltpu.SemaphoreType.DMA((n_lat - 1,)),
            pltpu.SemaphoreType.DMA((n_lat - 1,)),
            pltpu.SemaphoreType.DMA((n_lat - 1,)),
        ],
        compiler_params=pltpu.CompilerParams(
            collective_id=0, has_side_effects=True, vmem_limit_bytes=63 * 1024 * 1024
        ),
    )
    out, innovation = call(
        dest_tile, row_offset, col_offset, noisy_state, kernel_in, kernel_out,
        bias_in.reshape(1, chans), interp_weight, observed, obs_precision,
    )
    next_state = jnp.transpose(out.reshape(2, half, rows, width), (1, 2, 0, 3))
    return next_state.reshape(half, rows, cols), innovation


def solution(mesh):
    return jax.shard_map(
        functools.partial(body, mesh.shape["lat"], mesh.shape["lon"]),
        mesh=mesh,
        in_specs=(
            P(("grp", "ch"), "lat", "lon"),
            P(),
            P(),
            P(),
            P(("grp", "lat", "lon"), None, None),
            P(("grp", "lat", "lon"), "ch", None),
            P(("grp", "lat", "lon"), None),
            P(("grp", "lat", "lon")),
            P(("grp", "lat", "lon")),
            P(("grp", "lat", "lon")),
        ),
        out_specs=(P(("grp", "ch"), "lat", "lon"), P(("grp", "lat", "lon"), "ch", None)),
        check_vma=False,
    )
```

```python
import functools

import jax
import jax.numpy as jnp
from jax import lax
from jax.experimental import pallas as pl
from jax.experimental.pallas import tpu as pltpu
from jax.sharding import PartitionSpec as P

PH = 4
PW = 32
CAP = 2
HALO = 2
SIDE = 16
META = 16
GROUP = 8

keep_rate = 0.6
blend_rate = 0.4
guide_rate = 0.3

MESH = pl.DeviceIdType.MESH
F32 = jnp.float32
BF16 = jnp.bfloat16


def kernel(
    n_lat, n_lon, rows, width, half, blocks,
    dest, row_off, col_off, x_hbm, kin_hbm, kout_hbm, bias, weight_hbm, values_hbm, scale_hbm,
    out, inn_out,
    xv, xs, x_send, kin, kout, weight, values, scale_raw, scale, kfi, kfo, load_sem,
    both, X, X3, H3, pre, base, D, E, pay, R, G, GF, inn, inn_r, out_s, out_r, pulled_s,
    plan,
    halo_s, halo_r, pair_s, pair_r, pay_s, pay_r, inn_ss, inn_rs,
):
    lat, lon, ch = lax.axis_index("lat"), lax.axis_index("lon"), lax.axis_index("ch")
    other = 1 - ch
    chans = 2 * half
    obs = weight_hbm.shape[1]
    cells = PH * PW
    pitch = width + 2 * SIDE
    slots = n_lat * CAP
    px = rows * width
    lon_right = lax.rem(lon + ch, n_lon)
    lon_left = lax.rem(lon + n_lon - other, n_lon)
    has_up = lat > 0
    has_down = lat < n_lat - 1
    sibling = {"ch": other}

    def at(dlat, side):
        place = {"lat": lat + dlat}
        if side:
            place["lon"] = lon_right if side > 0 else lon_left
            place["ch"] = other
        return place

    loads = [
        pltpu.make_async_copy(src, dst, load_sem.at[i])
        for i, (src, dst) in enumerate(
            [(x_hbm, xv), (weight_hbm, weight), (values_hbm, values), (scale_hbm, scale_raw),
             (kin_hbm, kin), (kout_hbm, kout)]
        )
    ]
    for load in loads:
        load.start()
    barrier = pltpu.get_barrier_semaphore()

    def greet(place):
        pl.semaphore_signal(barrier, inc=1, device_id=place, device_id_type=MESH)

    for step in range(1, n_lat):
        greet({"lat": lax.rem(lat + step, n_lat)})
    greet(at(0, -1))
    greet(at(0, 1))

    @pl.when(has_up)
    def _():
        greet(at(-1, -1))
        greet(at(-1, 1))

    @pl.when(has_down)
    def _():
        greet(at(1, -1))
        greet(at(1, 1))

    def count_block(b, _):
        def earlier(e, rank):
            return rank + jnp.where(dest[e] == dest[b], 1, 0)

        plan[b] = dest[b] * CAP + lax.fori_loop(0, b, earlier, 0)
        return 0

    for b in range(blocks) if blocks <= 8 else ():
        rank = 0
        for e in range(b):
            rank = rank + jnp.where(dest[e] == dest[b], 1, 0)
        plan[b] = dest[b] * CAP + rank
    if blocks > 8:
        lax.fori_loop(0, blocks, count_block, 0)

    def pack_slot(s, _):
        def look(b, found):
            return jnp.where(plan[b] == s, b, found)

        found = lax.fori_loop(0, blocks, look, -1)
        source = jnp.maximum(found, 0)
        fill = jnp.where(found >= 0, 1.0, 0.0)
        w = (weight[source].astype(F32) * fill).astype(BF16)
        t = s // CAP
        k = s % CAP
        pay[t, k, 0:half] = w_half(w)
        pay[t, k, half:chans] = values[source]
        level = lax.broadcasted_iota(jnp.int32, (META, obs), 0)
        r0 = row_off[source].astype(F32)
        q0 = col_off[source].astype(F32)
        meta = jnp.where(level == 0, scale[pl.ds(source, 1), :], jnp.where(level == 1, r0, q0))
        pay[t, k, chans : chans + META] = meta.astype(BF16)
        return 0

    def w_half(w):
        return jnp.where(ch == 0, w[0:half].astype(F32), w[half:chans].astype(F32)).astype(BF16)

    loads[0].wait()
    for h in range(2):
        part = xv[:, :, h * width : (h + 1) * width].astype(F32)
        xs[h] = part.reshape(half * rows, width)
    for r in range(rows):
        both[ch, r] = xs[ch, pl.ds(r, half, stride=rows), :].astype(BF16)
        x_send[r] = xs[other, pl.ds(r, half, stride=rows), :].astype(BF16)

    tops = (lat + n_lat - 1) // n_lat
    bottoms = (2 * n_lat - 2 - lat) // n_lat
    pl.semaphore_wait(barrier, n_lat + 1 + 2 * tops + 2 * bottoms)

    def pair_copy(src, dst, i):
        return pltpu.make_async_remote_copy(
            src_ref=src, dst_ref=dst, send_sem=pair_s.at[i], recv_sem=pair_r.at[i],
            device_id=sibling, device_id_type=MESH,
        )

    reshard = pair_copy(x_send, both.at[ch], 0)
    reshard.start()
    for load in loads[1:4]:
        load.wait()
    scale[...] = scale_raw[...].astype(F32)
    lax.fori_loop(0, slots, pack_slot, 0)

    top, left = HALO, SIDE
    spans_r = {-1: (top, 0 + rows + top), 0: (top, top), 1: (top + rows - HALO, 0)}
    spans_c = {-1: (left, left + width), 0: (left, left), 1: (left + width - SIDE, 0)}
    size_r = {-1: HALO, 0: rows, 1: HALO}
    size_c = {-1: SIDE, 0: width, 1: SIDE}
    routes = [(0, -1), (0, 1), (-1, 0), (-1, -1), (-1, 1), (1, 0), (1, -1), (1, 1)]

    def halo_copy(buf, i, base_sem):
        dl, side = routes[i]
        sr, dr = spans_r[dl]
        sc, dc = spans_c[side]
        src = buf.at[pl.ds(sr, size_r[dl]), pl.ds(sc, size_c[side])]
        dst = buf.at[pl.ds(dr, size_r[dl]), pl.ds(dc, size_c[side])]
        return pltpu.make_async_remote_copy(
            src_ref=src, dst_ref=dst,
            send_sem=halo_s.at[base_sem + i], recv_sem=halo_r.at[base_sem + i],
            device_id=at(dl, side), device_id_type=MESH,
        )

    def halo_wait_recv(buf, i, base_sem):
        halo_copy(buf, i, base_sem).wait_recv()

    def guarded(dl, fn):
        if dl == 0:
            fn()
        else:
            pl.when(has_up if dl < 0 else has_down)(fn)

    def halo_start(buf, base_sem):
        for dl in (-1, 1, 0):
            def go(dl=dl):
                for i, route in enumerate(routes):
                    if route[0] == dl:
                        halo_copy(buf, i, base_sem).start()

            guarded(dl, go)

    def halo_finish(buf, base_sem, rows_of):
        for dl in rows_of:
            def go(dl=dl):
                for i, route in enumerate(routes):
                    if route[0] == dl:
                        halo_copy(buf, i, base_sem).wait_send()

            def got(dl=dl):
                for i, route in enumerate(routes):
                    if route[0] == dl:
                        halo_wait_recv(buf, i, base_sem)

            guarded(dl, go)
            guarded(-dl, got)

    def rim_conv(buf, base_sem, step):
        halo_finish(buf, base_sem, (0,))
        for r in range(HALO, HALO + rows):
            put_row(X3, r, buf[r].astype(F32))
        for r0 in range(HALO, rows, CH):
            step(r0)
        halo_finish(buf, base_sem, (-1, 1))
        for r in (0, 1, HALO + rows, HALO + rows + 1):
            put_row(X3, r, buf[r].astype(F32))
        for r0 in (0, rows):
            step(r0)

    CH = 2

    def clear_poles(buf):
        @pl.when(lat == 0)
        def _():
            buf[0:HALO] = jnp.zeros((HALO, pitch, chans), BF16)

        @pl.when(lat == n_lat - 1)
        def _():
            buf[rows + HALO : rows + 2 * HALO] = jnp.zeros((HALO, pitch, chans), BF16)

    def put_row(taps, r, v):
        taps[r * pitch : (r + 1) * pitch, 0:chans] = pltpu.roll(v, 1, 0).astype(BF16)
        taps[r * pitch : (r + 1) * pitch, chans : 2 * chans] = v.astype(BF16)
        taps[r * pitch : (r + 1) * pitch, 2 * chans :] = pltpu.roll(v, pitch - 1, 0).astype(BF16)

    def conv(taps, kmat, first, count):
        acc = None
        for a in range(3):
            part = jnp.dot(
                taps[(first + a) * pitch : (first + a + count) * pitch, :], kmat(a),
                preferred_element_type=F32,
            )
            acc = part if acc is None else acc + part
        return acc

    def mirrored(k, a):
        return jnp.concatenate([k[2 - a, 2], k[2 - a, 1], k[2 - a, 0]], axis=0)

    def edge_factor(r):
        if r == 0:
            return jnp.where(has_up, 1.0, 0.0)
        if r == rows + 1:
            return jnp.where(has_down, 1.0, 0.0)
        return None

    clear_poles(X)
    clear_poles(G)

    reshard.wait()
    for r in range(rows):
        X[top + r, left : left + width] = (
            jnp.concatenate([both[0, r], both[1, r]], axis=0).astype(F32).T.astype(BF16)
        )
    halo_start(X, 0)

    def pay_copy(i, step):
        peer = lax.rem(lat + step, n_lat)
        return pltpu.make_async_remote_copy(
            src_ref=pay.at[peer], dst_ref=R.at[lat, ch],
            send_sem=pay_s.at[i], recv_sem=pay_r.at[i],
            device_id={"lat": peer}, device_id_type=MESH,
        )

    for step in range(1, n_lat):
        pay_copy(step - 1, step).start()
    R[lat, ch] = pay[lat]
    for load in loads[4:]:
        load.wait()
    for a in range(3):
        for b in range(3):
            kfi[a, b * chans : (b + 1) * chans] = kin[a, b].astype(F32).T.astype(BF16)
            kfo[a, b * chans : (b + 1) * chans] = kout[a, b].astype(F32).T.astype(BF16)

    def hidden_rows(r0):
        acc = conv(X3, lambda a: kfi[a], r0, CH) + bias[...]
        pre[r0 * pitch : (r0 + CH) * pitch, :] = acc
        h = acc / (1.0 + jnp.exp(-acc))
        for i in range(CH):
            row = h[i * pitch : (i + 1) * pitch]
            f = edge_factor(r0 + i)
            if f is not None:
                row = row * f
            put_row(H3, r0 + i, row.astype(BF16).astype(F32))

    rim_conv(X, 0, hidden_rows)

    for r0 in range(0, rows, CH):
        acc = conv(H3, lambda a: kfo[a], r0, CH)
        for i in range(CH):
            r = r0 + i
            state = X[top + r, left : left + width].astype(F32)
            den = (state + acc[i * pitch + left : i * pitch + left + width]).astype(BF16)
            base[r * width : (r + 1) * width, :] = keep_rate * state + blend_rate * den.astype(F32)
            D[ch, :, r * width : (r + 1) * width] = den.astype(F32).T.astype(BF16)
    swap = pair_copy(D.at[ch], D.at[ch], 2)
    swap.start()

    for step in range(1, n_lat):
        pay_copy(step - 1, step).wait()
    forward = pair_copy(R.at[:, ch], R.at[:, ch], 1)
    forward.start()

    lane = lax.broadcasted_iota(jnp.int32, (1, cells), 1)
    cell_r = (lane // PW).astype(F32)
    cell_c = (lane % PW).astype(F32)

    def each_group(fn):
        if slots == GROUP:
            fn(0)
        else:
            lax.fori_loop(0, slots // GROUP, lambda g, _: fn(g) or 0, 0)

    def place_group(g):
        def place_rows(n, _):
            index = lax.broadcasted_iota(jnp.int32, (width, cells), 0) + n * width
            index = index.astype(F32)
            for i in range(GROUP):
                s = g * GROUP + i
                meta = R[s // CAP, ch, s % CAP, chans : chans + META].astype(F32)
                q = meta[2:3] + cell_c
                target = (meta[1:2] + cell_r) * width + q
                target = target + jnp.where(q >= width, float(px - width), 0.0)
                E[g, pl.ds(pl.multiple_of(n * width, width), width), i * cells : (i + 1) * cells] = (
                    jnp.where(index == target, 1.0, 0.0).astype(BF16)
                )
            return 0

        lax.fori_loop(0, 2 * rows, place_rows, 0)

    each_group(place_group)
    forward.wait()
    swap.wait()

    def observe_group(g):
        patches = jnp.dot(D[0], E[g, 0:px], preferred_element_type=F32) + jnp.dot(
            D[1], E[g, px : 2 * px], preferred_element_type=F32
        )
        patches = patches.astype(BF16)
        for i in range(GROUP):
            s = g * GROUP + i
            t = s // CAP
            k = s % CAP
            own = slice(i * cells, (i + 1) * cells)
            w = jnp.concatenate([R[t, 0, k, 0:half], R[t, 1, k, 0:half]], axis=0)
            val = jnp.concatenate([R[t, 0, k, half:chans], R[t, 1, k, half:chans]], axis=0)
            predicted = lax.dot_general(
                patches[:, own], w, (((1,), (1,)), ((), ())), preferred_element_type=F32
            )
            residual = predicted - val.astype(F32)
            inn[t, k] = jnp.where(ch == 0, residual[0:half], residual[half:chans]).astype(BF16)
            sc = R[t, 0, k, chans : chans + META].astype(F32)[0:1]
            weighted = (residual * sc).astype(BF16)
            pulled_s[g, :, own] = jnp.dot(weighted, w, preferred_element_type=F32).astype(BF16)

    each_group(observe_group)

    def spread_group(g):
        added = lax.dot_general(
            E[g, pl.ds(pl.multiple_of(ch * px, px), px)], pulled_s[g],
            (((1,), (1,)), ((), ())), preferred_element_type=F32,
        )
        if slots == GROUP:
            GF[...] = added
        else:
            GF[...] += added

    if slots != GROUP:
        GF[...] = jnp.zeros((px, chans), F32)
    each_group(spread_group)
    for r in range(rows):
        G[top + r, left : left + width] = GF[r * width : (r + 1) * width, :].astype(BF16)
    halo_start(G, 8)

    def inn_copy(i, step):
        peer = lax.rem(lat + step, n_lat)
        return pltpu.make_async_remote_copy(
            src_ref=inn.at[peer], dst_ref=inn_r.at[lat],
            send_sem=inn_ss.at[i], recv_sem=inn_rs.at[i],
            device_id={"lat": peer}, device_id_type=MESH,
        )

    for step in range(1, n_lat):
        inn_copy(step - 1, step).start()
    inn_r[lat] = inn[lat]

    def grad_rows(r0):
        back = conv(X3, lambda a: mirrored(kout, a), r0, CH)
        v = pre[r0 * pitch : (r0 + CH) * pitch, :]
        s = 1.0 / (1.0 + jnp.exp(-v))
        g = back * s * (1.0 + v * (1.0 - s))
        for i in range(CH):
            row = g[i * pitch : (i + 1) * pitch]
            f = edge_factor(r0 + i)
            if f is not None:
                row = row * f
            put_row(H3, r0 + i, row.astype(BF16).astype(F32))

    rim_conv(G, 8, grad_rows)
    for r0 in range(0, rows, CH):
        acc = conv(H3, lambda a: mirrored(kin, a), r0, CH)
        for i in range(CH):
            r = r0 + i
            own = slice(r * width, (r + 1) * width)
            grad = GF[own, :] + acc[i * pitch + left : i * pitch + left + width]
            res = (base[own, :] - guide_rate * grad).T
            out_s[0, pl.ds(r, half, stride=rows), :] = res[0:half]
            out_s[1, pl.ds(r, half, stride=rows), :] = res[half:chans]
    back_home = pair_copy(out_s.at[other], out_r, 3)
    back_home.start()
    out[ch] = out_s[ch]
    for step in range(1, n_lat):
        inn_copy(step - 1, step).wait()

    def fetch(b, _):
        slot = plan[b]
        inn_out[b] = inn_r[slot // CAP, slot % CAP]
        return 0

    lax.fori_loop(0, blocks, fetch, 0)
    back_home.wait()
    out[other] = out_r[...]


def body(n_lat, n_lon, noisy_state, kernel_in, bias_in, kernel_out, interp_weight, observed,
         obs_precision, dest_tile, row_offset, col_offset):
    half, rows, cols = noisy_state.shape
    chans = 2 * half
    width = cols // 2
    blocks, obs, cells = interp_weight.shape
    slots = n_lat * CAP
    pitch = width + 2 * SIDE
    px = rows * width
    vmem = pl.BlockSpec(memory_space=pltpu.VMEM)
    hbm = pl.BlockSpec(memory_space=pltpu.HBM)
    smem = pl.BlockSpec(memory_space=pltpu.SMEM)
    call = pl.pallas_call(
        functools.partial(kernel, n_lat, n_lon, rows, width, half, blocks),
        out_shape=(
            jax.ShapeDtypeStruct((2, half * rows, width), F32),
            jax.ShapeDtypeStruct((blocks, half, obs), BF16),
        ),
        in_specs=[smem] * 3 + [hbm] * 3 + [vmem] + [hbm] * 3,
        out_specs=(vmem, vmem),
        scratch_shapes=[
            pltpu.VMEM((half, rows, cols), BF16),
            pltpu.VMEM((2, half * rows, width), F32),
            pltpu.VMEM((rows, half, width), BF16),
            pltpu.VMEM(kernel_in.shape, BF16),
            pltpu.VMEM(kernel_out.shape, BF16),
            pltpu.VMEM(interp_weight.shape, BF16),
            pltpu.VMEM(observed.shape, BF16),
            pltpu.VMEM(obs_precision.shape, BF16),
            pltpu.VMEM(obs_precision.shape, F32),
            pltpu.VMEM((3, 3 * chans, chans), BF16),
            pltpu.VMEM((3, 3 * chans, chans), BF16),
            pltpu.SemaphoreType.DMA((6,)),
            pltpu.VMEM((2, rows, half, width), BF16),
            pltpu.VMEM((rows + 4, pitch, chans), BF16),
            pltpu.VMEM(((rows + 4) * pitch, 3 * chans), BF16),
            pltpu.VMEM(((rows + 2) * pitch, 3 * chans), BF16),
            pltpu.VMEM(((rows + 2) * pitch, chans), F32),
            pltpu.VMEM((px, chans), F32),
            pltpu.VMEM((2, chans, px), BF16),
            pltpu.VMEM((slots // GROUP, 2 * px, GROUP * cells), BF16),
            pltpu.VMEM((n_lat, CAP, chans + META, obs), BF16),
            pltpu.VMEM((n_lat, 2, CAP, chans + META, obs), BF16),
            pltpu.VMEM((rows + 4, pitch, chans), BF16),
            pltpu.VMEM((px, chans), F32),
            pltpu.VMEM((n_lat, CAP, half, obs), BF16),
            pltpu.VMEM((n_lat, CAP, half, obs), BF16),
            pltpu.VMEM((2, half * rows, width), F32),
            pltpu.VMEM((half * rows, width), F32),
            pltpu.VMEM((slots // GROUP, chans, GROUP * cells), BF16),
            pltpu.SMEM((blocks,), jnp.int32),
            pltpu.SemaphoreType.DMA((16,)),
            pltpu.SemaphoreType.DMA((16,)),
            pltpu.SemaphoreType.DMA((4,)),
            pltpu.SemaphoreType.DMA((4,)),
            pltpu.SemaphoreType.DMA((n_lat - 1,)),
            pltpu.SemaphoreType.DMA((n_lat - 1,)),
            pltpu.SemaphoreType.DMA((n_lat - 1,)),
            pltpu.SemaphoreType.DMA((n_lat - 1,)),
        ],
        compiler_params=pltpu.CompilerParams(
            collective_id=0, has_side_effects=True, vmem_limit_bytes=63 * 1024 * 1024
        ),
    )
    out, innovation = call(
        dest_tile, row_offset, col_offset, noisy_state, kernel_in, kernel_out,
        bias_in.reshape(1, chans), interp_weight, observed, obs_precision,
    )
    next_state = jnp.transpose(out.reshape(2, half, rows, width), (1, 2, 0, 3))
    return next_state.reshape(half, rows, cols), innovation


def solution(mesh):
    return jax.shard_map(
        functools.partial(body, mesh.shape["lat"], mesh.shape["lon"]),
        mesh=mesh,
        in_specs=(
            P(("grp", "ch"), "lat", "lon"),
            P(),
            P(),
            P(),
            P(("grp", "lat", "lon"), None, None),
            P(("grp", "lat", "lon"), "ch", None),
            P(("grp", "lat", "lon"), None),
            P(("grp", "lat", "lon")),
            P(("grp", "lat", "lon")),
            P(("grp", "lat", "lon")),
        ),
        out_specs=(P(("grp", "ch"), "lat", "lon"), P(("grp", "lat", "lon"), "ch", None)),
        check_vma=False,
    )
```
